32 devices in a mesh: dp: 16 (over z, y, x), vocab: 2 (over core).
Axes of the slice: x: 2, y: 2, z: 4, core: 2. Of those that a mesh axis runs over, the one named last changes fastest.
Arguments:
- hidden_states: bfloat16 [256, 3584], P('dp'), may hold values from -400 to 400
- targets: int32 [256], P('dp'), may hold values from 0 to 49151
- out_weight: bfloat16 [3584, 49152], P(None, ('dp', 'vocab')), may hold values from -5 to 5
Outputs:
- token_loss: float32 [256], P('dp')
- loss_mean: float32 [], replicated
The draws below stay inside these ranges and needn't reach their ends.
All inputs are finite; a program needn't handle non-finite values.
Results may differ from the reference program's by a relative error of at most 0.0003.
Values may be sent and summed in bfloat16 or wider, within the bound.
No kernel may reach another device: no remote copies, remote signals or barrier semaphores. Data moves between devices by JAX's collectives and lax.ppermute only.
A program may use at most 64 MiB of HBM per device.

```python
import math
import jax
import jax.numpy as jnp
from jax import lax

D = 3584
VOC_DEV = 1536
TOK_DEV = 16
VOCAB = 49152
TOKENS = 256


def column_draw(key, column_ids):

    def single(column):
        column_key = jax.random.fold_in(jax.random.fold_in(key, 11), column)
        spread = jnp.exp(jax.random.uniform(jax.random.fold_in(column_key, 1), (), jnp.float32, math.log(0.7), math.log(7.0)))
        values = jnp.clip(jax.random.normal(jax.random.fold_in(column_key, 2), (D,), jnp.float32), -5.0, 5.0)
        return values * spread / math.sqrt(D)
    return jax.vmap(single)(column_ids)


def draw_out_weight(key, part):
    column_ids = jnp.arange(VOCAB, dtype=jnp.int32).reshape(VOCAB // VOC_DEV, VOC_DEV)
    blocks = lax.map(lambda ids: column_draw(key, ids).T, column_ids)
    return jnp.transpose(blocks, (1, 0, 2)).reshape(D, VOCAB).astype(jnp.bfloat16)


def draw_hidden_states(key, part):
    base = jnp.clip(jax.random.normal(jax.random.fold_in(key, 21), (TOKENS, D), jnp.float32), -5.0, 5.0)
    return base.astype(jnp.bfloat16)


def with_ends(entries, key, least, high):
    shape = entries.shape
    spot = [jax.random.randint(jax.random.fold_in(key, axis), (), 0, shape[axis]) for axis in range(len(shape))]
    entries = entries.at[tuple(spot)].set(least)
    longest = shape.index(max(shape))
    spot[longest] = (spot[longest] + 1) % shape[longest]
    return entries.at[tuple(spot)].set(high)


def setup_inputs(seed: int = 0) -> dict:
    arg_keys = jax.random.split(jax.random.key(seed), 4)
    return {
        "hidden_states": draw_hidden_states(jax.random.fold_in(arg_keys[3], 71), 0),
        "targets": with_ends(jax.random.randint(arg_keys[1], (TOKENS,), 0, VOCAB), jax.random.fold_in(arg_keys[1], 1), 0, VOCAB - 1).astype(jnp.int32),
        "out_weight": draw_out_weight(jax.random.fold_in(arg_keys[3], 71), 0),
    }


def reference(hidden_states, targets, out_weight):
    def per_block(pair):
        states, labels = pair
        logits = jnp.dot(states, out_weight, preferred_element_type=jnp.float32)
        row_top = jnp.max(logits, axis=1)
        log_norm = row_top + jnp.log(jnp.sum(jnp.exp(logits - row_top[:, None]), axis=1))
        picked = jnp.take_along_axis(logits, labels[:, None].astype(jnp.int32), axis=1)[:, 0]
        return log_norm - picked

    token_loss = lax.map(per_block, (hidden_states.reshape(TOKENS // TOK_DEV, TOK_DEV, D), targets.reshape(TOKENS // TOK_DEV, TOK_DEV)))
    token_loss = token_loss.reshape(TOKENS)
    return token_loss, jnp.mean(token_loss)
```

```python
import jax
import jax.numpy as jnp
from jax import lax
from jax.sharding import PartitionSpec as P

LANES = 128
BASE = 256
DIGITS = 3


def everywhere(block, axes, count):
    copies = jnp.broadcast_to(block[None], (count,) + block.shape)
    return lax.all_to_all(copies, axes, 0, 0)


def shards(hidden_states, targets, out_weight):
    features, vocab_cols = out_weight.shape
    local_tokens = hidden_states.shape[0]
    groups, cores = lax.axis_size("dp"), lax.axis_size("vocab")
    group, core = lax.axis_index("dp"), lax.axis_index("vocab")
    share = local_tokens // cores
    tokens = groups * local_tokens

    digits = [(targets // BASE**i) % BASE for i in range(DIGITS)]
    digits = jnp.stack(digits, axis=1).astype(hidden_states.dtype)
    digits = jnp.pad(digits, ((0, 0), (0, LANES - DIGITS)))
    rows = jnp.concatenate([hidden_states, digits], axis=1)
    mine = lax.dynamic_slice_in_dim(rows, core * share, share, 0)
    mine = everywhere(mine, "dp", groups).reshape(groups * share, -1)
    swap = [(i, (i + 1) % cores) for i in range(cores)]
    other = lax.ppermute(mine, "vocab", swap)
    both = jnp.concatenate([mine, other], axis=0)
    states = both[:, :features]
    labels = both[:, features : features + DIGITS].astype(jnp.int32)
    labels = sum(labels[:, i] * BASE**i for i in range(DIGITS))

    logits = jnp.dot(states, out_weight, preferred_element_type=jnp.float32)
    start = (group * cores + core) * vocab_cols
    columns = start + lax.broadcasted_iota(jnp.int32, logits.shape, 1)
    is_target = columns == labels[:, None]
    picked = jnp.sum(jnp.where(is_target, logits, 0.0), axis=1)
    top = jnp.max(logits, axis=1)
    norm = top + jnp.log(jnp.sum(jnp.exp(logits - top[:, None]), axis=1))
    stats = jnp.stack([norm, picked])
    halves = stats.reshape(2, cores, groups * share)
    halves = jnp.where(core == 0, halves, halves[:, ::-1])
    stats = halves.reshape(2, tokens)

    stats = everywhere(stats, ("dp", "vocab"), groups * cores)
    norms = stats[:, 0]
    top = jnp.max(norms, axis=0)
    log_norm = top + jnp.log(jnp.sum(jnp.exp(norms - top), axis=0))
    loss = log_norm - jnp.sum(stats[:, 1], axis=0)
    loss = loss.reshape(cores, groups, share)
    token_loss = lax.dynamic_slice_in_dim(loss, group, 1, 1)
    return token_loss.reshape(local_tokens), jnp.sum(loss) / tokens


def solution(mesh):
    placed = (P("dp", None), P("dp"), P(None, ("dp", "vocab")))
    return jax.shard_map(
        shards, mesh=mesh, in_specs=placed, out_specs=(P("dp"), P()), check_vma=False
    )
```

```python
import functools

import jax
import jax.numpy as jnp
from jax import lax
from jax.experimental import pallas as pl
from jax.experimental.pallas import tpu as pltpu
from jax.sharding import PartitionSpec as P

LANES = 128
SUB = 8
BASE = 256
DIGITS = 3
TILE = 256
VMEM = pl.BlockSpec(memory_space=pltpu.VMEM)
LIMIT = pltpu.CompilerParams(vmem_limit_bytes=20 * 2**20)
HBM = pl.BlockSpec(memory_space=pltpu.HBM)
CHUNKS = 8


def near(array):
    return pltpu.with_memory_space_constraint(array, pltpu.VMEM)


def far(array):
    return pltpu.with_memory_space_constraint(array, pltpu.HBM)


def orders(groups):
    bits = [1 << b for b in reversed(range(groups.bit_length() - 1))]
    return (bits[:-2] + bits[-1:] + bits[-2:-1], bits)


def place(order, j):
    where = 0
    for b, k in enumerate(order):
        where ^= k * ((j >> b) & 1)
    return where


def pack_kernel(share, targets_hbm, states_hbm, *refs):
    piece_refs, (targets_ref, states_ref, sems) = refs[:-3], refs[-3:]
    core = lax.axis_index("vocab")
    first = pl.multiple_of(core * share, share)
    copies = (
        pltpu.make_async_copy(targets_hbm, targets_ref, sems.at[0]),
        pltpu.make_async_copy(
            states_hbm.at[pl.ds(first, share), :], states_ref, sems.at[1]
        ),
    )
    for copy in copies:
        copy.start()
    for copy in copies:
        copy.wait()
    block = states_ref[...]
    row = lax.broadcasted_iota(jnp.int32, (share, LANES), 0)
    lane = lax.broadcasted_iota(jnp.int32, (share, LANES), 1)
    label = jnp.zeros((share, LANES), jnp.int32)
    for t in range(share):
        label = jnp.where(row == t, targets_ref[first + t], label)
    digits = jnp.zeros((share, LANES), jnp.int32)
    for d in range(DIGITS):
        digits = jnp.where(lane == d, (label >> (8 * d)) & (BASE - 1), digits)
    digits = digits.astype(jnp.float32).astype(block.dtype)
    at = 0
    for c, ref in enumerate(piece_refs):
        last = c == len(piece_refs) - 1
        width = ref.shape[1] - (LANES if last else 0)
        ref[:, :width] = block[:, at : at + width]
        at += width
        if last:
            ref[:, width:] = digits


def load_kernel(source, piece_ref, target, again_ref, sems):
    rows = source.shape[0] // CHUNKS
    copies = []
    for n in range(CHUNKS):
        part = pl.ds(n * rows, rows)
        copies.append(
            pltpu.make_async_copy(source.at[part], target.at[part], sems.at[n])
        )
        copies[-1].start()
    again_ref[...] = piece_ref[...]
    for copy in copies:
        copy.wait()


def score_kernel(plan, flip, *refs):
    pieces, rest = refs[: 2 * len(plan)], list(refs[2 * len(plan) :])
    weight_ref = rest.pop(0)
    before_ref = rest.pop(0) if flip else None
    out_ref, rows_ref, logits_ref, stats_ref = rest
    features, vocab_cols = weight_ref.shape
    rows = rows_ref.shape[0]
    group, core = lax.axis_index("dp"), lax.axis_index("vocab")
    cores = lax.axis_size("vocab")
    at = 0
    for c, order in enumerate(plan):
        early, late = pieces[2 * c : 2 * c + 2]
        width = early.shape[1]
        for j in range(rows // SUB):
            to = place(order, j) * SUB
            ref = early if j < rows // SUB // 2 else late
            at_row = j * SUB % (rows // 2)
            rows_ref[to : to + SUB, at : at + width] = ref[at_row : at_row + SUB, :]
        at += width
    states = rows_ref[:, :features]

    def multiply(n, top):
        columns = pl.ds(pl.multiple_of(n * TILE, TILE), TILE)
        part = jnp.dot(
            states, weight_ref[:, columns], preferred_element_type=jnp.float32
        )
        logits_ref[:, columns] = part
        for k in range(TILE // LANES):
            top = jnp.maximum(top, part[:, k * LANES : (k + 1) * LANES])
        return top

    top = jnp.full((rows, LANES), -jnp.inf, jnp.float32)
    top = lax.fori_loop(0, vocab_cols // TILE, multiply, top)
    top = jnp.max(top, axis=1, keepdims=True)
    digits = rows_ref[:, features:].astype(jnp.float32)
    lane = lax.broadcasted_iota(jnp.int32, (rows, LANES), 1)
    scale = jnp.where(lane == 0, 1.0, jnp.where(lane == 1, 256.0, 65536.0))
    scale = jnp.where(lane < DIGITS, scale, 0.0)
    label = jnp.sum(digits * scale, axis=1, keepdims=True).astype(jnp.int32)
    start = (group * cores + core) * vocab_cols
    offset = lane + start - label

    total = jnp.zeros((rows, LANES), jnp.float32)
    picked = jnp.zeros((rows, LANES), jnp.float32)
    for n in range(vocab_cols // LANES):
        part = logits_ref[:, n * LANES : (n + 1) * LANES]
        total = total + jnp.exp(part - top)
        picked = picked + jnp.where(offset == -n * LANES, part, 0.0)
    norm = top + jnp.log(jnp.sum(total, axis=1, keepdims=True))
    picked = jnp.sum(picked, axis=1, keepdims=True)
    stats = jnp.where(lane == 0, norm, jnp.where(lane == 1, picked, 0.0))
    for j in range(rows // SUB):
        to = pl.multiple_of((group ^ j) * SUB, SUB)
        stats_ref[pl.ds(to, SUB), :] = stats[j * SUB : (j + 1) * SUB, :]
    stats = stats_ref[...].T[:2, :]
    if not flip:
        out_ref[...] = stats
        return
    before = before_ref[...]
    low = jnp.where(core == 0, before, stats)
    high = jnp.where(core == 0, stats, before)
    out_ref[:, 0:1, :] = jnp.broadcast_to(low[0:1][None], (out_ref.shape[0], 1, rows))
    out_ref[:, 1:2, :] = jnp.broadcast_to(high[0:1][None], (out_ref.shape[0], 1, rows))
    out_ref[:, 2:3, :] = jnp.broadcast_to(low[1:2][None], (out_ref.shape[0], 1, rows))
    out_ref[:, 3:4, :] = jnp.broadcast_to(high[1:2][None], (out_ref.shape[0], 1, rows))


def finish_kernel(share, stats_ref, token_ref, mean_ref):
    group = lax.axis_index("dp")
    stats = stats_ref[...]
    length = stats.shape[-1]
    top = jnp.max(stats, axis=0)
    total = jnp.sum(jnp.exp(stats - top[None]), axis=0)
    log_norm = top + jnp.log(total)
    picked = jnp.sum(stats, axis=0)
    loss = log_norm[0:2] - picked[2:4]
    mean_ref[...] = jnp.sum(loss, keepdims=True) / (2 * length)
    lane = lax.broadcasted_iota(jnp.int32, (1, length), 1)
    low = pltpu.roll(loss[0:1], (length - group * share) % length, 1)
    high = pltpu.roll(loss[1:2], (length + share - group * share) % length, 1)
    token_ref[...] = jnp.where(lane < share, low, high)[:, : 2 * share]


def shards(hidden_states, targets, out_weight):
    features, vocab_cols = out_weight.shape
    local_tokens = hidden_states.shape[0]
    groups, cores = lax.axis_size("dp"), lax.axis_size("vocab")
    share = local_tokens // cores
    half = groups * share
    dtype = hidden_states.dtype
    plan = orders(groups)
    cut = features // len(plan) // LANES * LANES
    widths = [cut] * (len(plan) - 1)
    widths.append(features - sum(widths) + LANES)

    pieces = pl.pallas_call(
        functools.partial(pack_kernel, share),
        out_shape=[jax.ShapeDtypeStruct((share, w), dtype) for w in widths],
        in_specs=[HBM, HBM],
        out_specs=[VMEM] * len(widths),
        scratch_shapes=[
            pltpu.SMEM((local_tokens,), jnp.int32),
            pltpu.VMEM((share, features), dtype),
            pltpu.SemaphoreType.DMA((2,)),
        ],
        compiler_params=LIMIT,
        name="pack",
    )(far(targets), far(hidden_states))

    weight, again = pl.pallas_call(
        load_kernel,
        out_shape=[
            jax.ShapeDtypeStruct(out_weight.shape, dtype),
            jax.ShapeDtypeStruct(pieces[0].shape, dtype),
        ],
        in_specs=[HBM, VMEM],
        out_specs=[VMEM, VMEM],
        scratch_shapes=[pltpu.SemaphoreType.DMA((CHUNKS,))],
        compiler_params=LIMIT,
        cost_estimate=pl.CostEstimate(
            flops=2 * half * features * vocab_cols, bytes_accessed=0, transcendentals=0
        ),
        name="load",
    )(far(out_weight), pieces[0])

    mine = [[piece] for piece in pieces]
    for step in range(len(plan[0])):
        for c, order in enumerate(plan):
            flips = [(i, i ^ order[step]) for i in range(groups)]
            whole = jnp.concatenate(mine[c], axis=0)
            mine[c] = [whole, lax.ppermute(whole, "dp", flips)]
            if step == 0 and c == 0:
                mine[c][0] = again
    mine = [part for pair in mine for part in pair]
    swap = [(i, (i + 1) % cores) for i in range(cores)]
    other = [lax.ppermute(part, "vocab", swap) for part in mine]

    weight = near(weight)
    cost = pl.CostEstimate(
        flops=2 * half * features * vocab_cols,
        bytes_accessed=2 * half * features,
        transcendentals=half * vocab_cols,
    )

    def score(pieces, before):
        flip = before is not None
        shape = (groups * cores, 4, half) if flip else (2, half)
        extra = [before] if flip else []
        return pl.pallas_call(
            functools.partial(score_kernel, plan, flip),
            out_shape=jax.ShapeDtypeStruct(shape, jnp.float32),
            in_specs=[VMEM] * (len(pieces) + 1 + len(extra)),
            out_specs=VMEM,
            scratch_shapes=[
                pltpu.VMEM((half, features + LANES), dtype),
                pltpu.VMEM((half, vocab_cols), jnp.float32),
                pltpu.VMEM((half, LANES), jnp.float32),
            ],
            cost_estimate=cost,
            compiler_params=LIMIT,
            name="score_other" if flip else "score_mine",
        )(*[near(p) for p in pieces], weight, *extra)

    stats = score(other, score(mine, None))
    stats = lax.all_to_all(stats, ("dp", "vocab"), 0, 0)
    token_loss, loss_mean = pl.pallas_call(
        functools.partial(finish_kernel, share),
        out_shape=[
            jax.ShapeDtypeStruct((1, local_tokens), jnp.float32),
            jax.ShapeDtypeStruct((1, 1), jnp.float32),
        ],
        in_specs=[VMEM],
        out_specs=[VMEM, VMEM],
        compiler_params=LIMIT,
        name="finish",
    )(stats)
    return token_loss.reshape(local_tokens), loss_mean.reshape(())


def solution(mesh):
    placed = (P("dp", None), P("dp"), P(None, ("dp", "vocab")))
    return jax.shard_map(
        shards, mesh=mesh, in_specs=placed, out_specs=(P("dp"), P()), check_vma=False
    )
```

```python
import functools

import jax
import jax.numpy as jnp
from jax import lax
from jax.experimental import pallas as pl
from jax.experimental.pallas import tpu as pltpu
from jax.sharding import PartitionSpec as P

LANES = 128
SUB = 8
BASE = 256
DIGITS = 3
LOADS = (2, 1)
TILE = 256
VMEM = pl.BlockSpec(memory_space=pltpu.VMEM)
LIMIT = pltpu.CompilerParams(vmem_limit_bytes=20 * 2**20)
HBM = pl.BlockSpec(memory_space=pltpu.HBM)
CHUNKS = 8


def near(array):
    return pltpu.with_memory_space_constraint(array, pltpu.VMEM)


def far(array):
    return pltpu.with_memory_space_constraint(array, pltpu.HBM)


def orders(groups):
    bits = [1 << b for b in reversed(range(groups.bit_length() - 1))]
    return (bits, bits[-1:] + bits[:-1])


def place(order, j):
    where = 0
    for b, k in enumerate(order):
        where ^= k * ((j >> b) & 1)
    return where


def pack_kernel(share, targets_hbm, states_hbm, *refs):
    piece_refs, (targets_ref, states_ref, sems) = refs[:-3], refs[-3:]
    core = lax.axis_index("vocab")
    first = pl.multiple_of(core * share, share)
    copies = (
        pltpu.make_async_copy(targets_hbm, targets_ref, sems.at[0]),
        pltpu.make_async_copy(
            states_hbm.at[pl.ds(first, share), :], states_ref, sems.at[1]
        ),
    )
    for copy in copies:
        copy.start()
    for copy in copies:
        copy.wait()
    block = states_ref[...]
    row = lax.broadcasted_iota(jnp.int32, (share, LANES), 0)
    lane = lax.broadcasted_iota(jnp.int32, (share, LANES), 1)
    label = jnp.zeros((share, LANES), jnp.int32)
    for t in range(share):
        label = jnp.where(row == t, targets_ref[first + t], label)
    digits = jnp.zeros((share, LANES), jnp.int32)
    for d in range(DIGITS):
        digits = jnp.where(lane == d, (label >> (8 * d)) & (BASE - 1), digits)
    digits = digits.astype(jnp.float32).astype(block.dtype)
    at = 0
    for c, ref in enumerate(piece_refs):
        last = c == len(piece_refs) - 1
        width = ref.shape[1] - (LANES if last else 0)
        ref[:, :width] = block[:, at : at + width]
        at += width
        if last:
            ref[:, width:] = digits


def load_kernel(part, source, piece_ref, *refs):
    target, again_ref, sems = refs[-3:]
    first, size = part
    rows = size // CHUNKS
    copies = []
    for n in range(CHUNKS):
        span = pl.ds(first + n * rows, rows)
        copies.append(
            pltpu.make_async_copy(source.at[span], target.at[span], sems.at[n])
        )
        copies[-1].start()
    again_ref[...] = piece_ref[...]
    for copy in copies:
        copy.wait()


def load(part, source, piece, target):
    first = target is None
    return pl.pallas_call(
        functools.partial(load_kernel, part),
        out_shape=[
            jax.ShapeDtypeStruct(source.shape, source.dtype),
            jax.ShapeDtypeStruct(piece.shape, piece.dtype),
        ],
        in_specs=[HBM, VMEM] + ([] if first else [VMEM]),
        out_specs=[VMEM, VMEM],
        scratch_shapes=[pltpu.SemaphoreType.DMA((CHUNKS,))],
        input_output_aliases={} if first else {2: 0},
        compiler_params=LIMIT,
        cost_estimate=pl.CostEstimate(
            flops=2 * part[1] * source.shape[1] * 2 * LANES,
            bytes_accessed=0,
            transcendentals=0,
        ),
        name=f"load_{part[0]}",
    )(far(source), piece, *([] if first else [near(target)]))


def score_kernel(plan, flip, *refs):
    pieces, rest = refs[: 2 * len(plan)], list(refs[2 * len(plan) :])
    weight_ref = rest.pop(0)
    before_ref = rest.pop(0) if flip else None
    out_ref, rows_ref, logits_ref, stats_ref = rest
    features, vocab_cols = weight_ref.shape
    rows = rows_ref.shape[0]
    group, core = lax.axis_index("dp"), lax.axis_index("vocab")
    cores = lax.axis_size("vocab")
    at = 0
    for c, order in enumerate(plan):
        early, late = pieces[2 * c : 2 * c + 2]
        width = early.shape[1]
        for j in range(rows // SUB):
            to = place(order, j) * SUB
            ref = early if j < rows // SUB // 2 else late
            at_row = j * SUB % (rows // 2)
            rows_ref[to : to + SUB, at : at + width] = ref[at_row : at_row + SUB, :]
        at += width
    states = rows_ref[:, :features]

    def multiply(n, top):
        columns = pl.ds(pl.multiple_of(n * TILE, TILE), TILE)
        part = jnp.dot(
            states, weight_ref[:, columns], preferred_element_type=jnp.float32
        )
        logits_ref[:, columns] = part
        for k in range(TILE // LANES):
            top = jnp.maximum(top, part[:, k * LANES : (k + 1) * LANES])
        return top

    top = jnp.full((rows, LANES), -jnp.inf, jnp.float32)
    top = lax.fori_loop(0, vocab_cols // TILE, multiply, top, unroll=True)
    top = jnp.max(top, axis=1, keepdims=True)
    digits = rows_ref[:, features:].astype(jnp.float32)
    lane = lax.broadcasted_iota(jnp.int32, (rows, LANES), 1)
    scale = jnp.where(lane == 0, 1.0, jnp.where(lane == 1, 256.0, 65536.0))
    scale = jnp.where(lane < DIGITS, scale, 0.0)
    label = jnp.sum(digits * scale, axis=1, keepdims=True).astype(jnp.int32)
    start = (group * cores + core) * vocab_cols
    offset = lane + start - label

    total = jnp.zeros((rows, LANES), jnp.float32)
    picked = jnp.zeros((rows, LANES), jnp.float32)
    for n in range(vocab_cols // LANES):
        part = logits_ref[:, n * LANES : (n + 1) * LANES]
        total = total + jnp.exp(part - top)
        picked = picked + jnp.where(offset == -n * LANES, part, 0.0)
    norm = top + jnp.log(jnp.sum(total, axis=1, keepdims=True))
    picked = jnp.sum(picked, axis=1, keepdims=True)
    stats = jnp.where(lane == 0, norm, jnp.where(lane == 1, picked, 0.0))
    for j in range(rows // SUB):
        to = pl.multiple_of((group ^ j) * SUB, SUB)
        stats_ref[pl.ds(to, SUB), :] = stats[j * SUB : (j + 1) * SUB, :]
    stats = stats_ref[...].T[:2, :]
    if not flip:
        out_ref[...] = stats
        return
    before = before_ref[...]
    low = jnp.where(core == 0, before, stats)
    high = jnp.where(core == 0, stats, before)
    out_ref[:, 0:1, :] = jnp.broadcast_to(low[0:1][None], (out_ref.shape[0], 1, rows))
    out_ref[:, 1:2, :] = jnp.broadcast_to(high[0:1][None], (out_ref.shape[0], 1, rows))
    out_ref[:, 2:3, :] = jnp.broadcast_to(low[1:2][None], (out_ref.shape[0], 1, rows))
    out_ref[:, 3:4, :] = jnp.broadcast_to(high[1:2][None], (out_ref.shape[0], 1, rows))


def finish_kernel(share, stats_ref, token_ref, mean_ref):
    group = lax.axis_index("dp")
    stats = stats_ref[...]
    length = stats.shape[-1]
    top = jnp.max(stats, axis=0)
    total = jnp.sum(jnp.exp(stats - top[None]), axis=0)
    log_norm = top + jnp.log(total)
    picked = jnp.sum(stats, axis=0)
    loss = log_norm[0:2] - picked[2:4]
    mean_ref[...] = jnp.sum(loss, keepdims=True) / (2 * length)
    lane = lax.broadcasted_iota(jnp.int32, (1, length), 1)
    low = pltpu.roll(loss[0:1], (length - group * share) % length, 1)
    high = pltpu.roll(loss[1:2], (length + share - group * share) % length, 1)
    token_ref[...] = jnp.where(lane < share, low, high)[:, : 2 * share]


def shards(hidden_states, targets, out_weight):
    features, vocab_cols = out_weight.shape
    local_tokens = hidden_states.shape[0]
    groups, cores = lax.axis_size("dp"), lax.axis_size("vocab")
    share = local_tokens // cores
    half = groups * share
    dtype = hidden_states.dtype
    plan = orders(groups)
    cut = features // len(plan) // LANES * LANES
    widths = [cut] * (len(plan) - 1)
    widths.append(features - sum(widths) + LANES)

    pieces = pl.pallas_call(
        functools.partial(pack_kernel, share),
        out_shape=[jax.ShapeDtypeStruct((share, w), dtype) for w in widths],
        in_specs=[HBM, HBM],
        out_specs=[VMEM] * len(widths),
        scratch_shapes=[
            pltpu.SMEM((local_tokens,), jnp.int32),
            pltpu.VMEM((share, features), dtype),
            pltpu.SemaphoreType.DMA((2,)),
        ],
        compiler_params=LIMIT,
        name="pack",
    )(far(targets), far(hidden_states))

    steps = len(plan[0])
    weight = None
    mine = [[piece] for piece in pieces]
    done = 0
    for step in range(steps):
        for c, order in enumerate(plan):
            flips = [(i, i ^ order[step]) for i in range(groups)]
            whole = jnp.concatenate(mine[c], axis=0)
            mine[c] = [whole, lax.ppermute(whole, "dp", flips)]
        if step < len(LOADS):
            size = int((features - done) / LOADS[step])
            size = size // (SUB * CHUNKS) * SUB * CHUNKS
            weight, mine[-1][0] = load((done, size), out_weight, whole, weight)
            done += size
    mine = [part for pair in mine for part in pair]
    swap = [(i, (i + 1) % cores) for i in range(cores)]
    other = [lax.ppermute(part, "vocab", swap) for part in mine]

    weight = near(weight)
    cost = pl.CostEstimate(
        flops=2 * half * features * vocab_cols,
        bytes_accessed=2 * half * features,
        transcendentals=half * vocab_cols,
    )

    def score(pieces, before):
        flip = before is not None
        shape = (groups * cores, 4, half) if flip else (2, half)
        extra = [before] if flip else []
        return pl.pallas_call(
            functools.partial(score_kernel, plan, flip),
            out_shape=jax.ShapeDtypeStruct(shape, jnp.float32),
            in_specs=[VMEM] * (len(pieces) + 1 + len(extra)),
            out_specs=VMEM,
            scratch_shapes=[
                pltpu.VMEM((half, features + LANES), dtype),
                pltpu.VMEM((half, vocab_cols), jnp.float32),
                pltpu.VMEM((half, LANES), jnp.float32),
            ],
            cost_estimate=cost,
            compiler_params=LIMIT,
            name="score_other" if flip else "score_mine",
        )(*[near(p) for p in pieces], weight, *extra)

    stats = score(other, score(mine, None))
    stats = lax.all_to_all(stats, ("dp", "vocab"), 0, 0)
    token_loss, loss_mean = pl.pallas_call(
        functools.partial(finish_kernel, share),
        out_shape=[
            jax.ShapeDtypeStruct((1, local_tokens), jnp.float32),
            jax.ShapeDtypeStruct((1, 1), jnp.float32),
        ],
        in_specs=[VMEM],
        out_specs=[VMEM, VMEM],
        compiler_params=LIMIT,
        name="finish",
    )(stats)
    return token_loss.reshape(local_tokens), loss_mean.reshape(())


def solution(mesh):
    placed = (P("dp", None), P("dp"), P(None, ("dp", "vocab")))
    return jax.shard_map(
        shards, mesh=mesh, in_specs=placed, out_specs=(P("dp"), P()), check_vma=False
    )
```

```python
import functools

import jax
import jax.numpy as jnp
from jax import lax
from jax.experimental import pallas as pl
from jax.experimental.pallas import tpu as pltpu
from jax.sharding import PartitionSpec as P

LANES = 128
SUB = 8
BASE = 256
DIGITS = 3
ORDER = (1, 2, 3)
SHARE = 0.6
STEPS = (0, 1)
TILE = 256
VMEM = pl.BlockSpec(memory_space=pltpu.VMEM)
LIMIT = pltpu.CompilerParams(vmem_limit_bytes=20 * 2**20)
HBM = pl.BlockSpec(memory_space=pltpu.HBM)
CHUNKS = 8


def near(array):
    return pltpu.with_memory_space_constraint(array, pltpu.VMEM)


def far(array):
    return pltpu.with_memory_space_constraint(array, pltpu.HBM)


def orders(groups):
    bits = [1 << b for b in reversed(range(groups.bit_length() - 1))]
    return (bits, bits[:-2] + bits[-1:] + bits[-2:-1])


def place(order, j):
    where = 0
    for b, k in enumerate(order):
        where ^= k * ((j >> b) & 1)
    return where


def pack_kernel(share, targets_hbm, states_hbm, *refs):
    piece_refs, (targets_ref, states_ref, sems) = refs[:-3], refs[-3:]
    core = lax.axis_index("vocab")
    first = pl.multiple_of(core * share, share)
    copies = (
        pltpu.make_async_copy(targets_hbm, targets_ref, sems.at[0]),
        pltpu.make_async_copy(
            states_hbm.at[pl.ds(first, share), :], states_ref, sems.at[1]
        ),
    )
    for copy in copies:
        copy.start()
    for copy in copies:
        copy.wait()
    block = states_ref[...]
    row = lax.broadcasted_iota(jnp.int32, (share, LANES), 0)
    lane = lax.broadcasted_iota(jnp.int32, (share, LANES), 1)
    label = jnp.zeros((share, LANES), jnp.int32)
    for t in range(share):
        label = jnp.where(row == t, targets_ref[first + t], label)
    digits = jnp.zeros((share, LANES), jnp.int32)
    for d in range(DIGITS):
        digits = jnp.where(lane == d, (label >> (8 * d)) & (BASE - 1), digits)
    digits = digits.astype(jnp.float32).astype(block.dtype)
    at = 0
    for c, ref in enumerate(piece_refs):
        last = c == len(piece_refs) - 1
        width = ref.shape[1] - (LANES if last else 0)
        ref[:, :width] = block[:, at : at + width]
        at += width
        if last:
            ref[:, width:] = digits


def load_kernel(part, source, piece_ref, *refs):
    target, again_ref, sems = refs[-3:]
    first, size = part
    rows = size // CHUNKS
    copies = []
    for n in range(CHUNKS):
        span = pl.ds(first + n * rows, rows)
        copies.append(
            pltpu.make_async_copy(source.at[span], target.at[span], sems.at[n])
        )
        copies[-1].start()
    again_ref[...] = piece_ref[...]
    for copy in copies:
        copy.wait()


def load(part, source, piece, target):
    first = target is None
    return pl.pallas_call(
        functools.partial(load_kernel, part),
        out_shape=[
            jax.ShapeDtypeStruct(source.shape, source.dtype),
            jax.ShapeDtypeStruct(piece.shape, piece.dtype),
        ],
        in_specs=[HBM, VMEM] + ([] if first else [VMEM]),
        out_specs=[VMEM, VMEM],
        scratch_shapes=[pltpu.SemaphoreType.DMA((CHUNKS,))],
        input_output_aliases={} if first else {2: 0},
        compiler_params=LIMIT,
        cost_estimate=pl.CostEstimate(
            flops=2 * part[1] * source.shape[1] * 2 * LANES,
            bytes_accessed=0,
            transcendentals=0,
        ),
        name=f"load_{part[0]}",
    )(far(source), piece, *([] if first else [near(target)]))


def score_kernel(plan, flip, *refs):
    pieces, rest = refs[: 2 * len(plan)], list(refs[2 * len(plan) :])
    weight_ref = rest.pop(0)
    before_ref = rest.pop(0) if flip else None
    out_ref, rows_ref, logits_ref, stats_ref = rest
    features, vocab_cols = weight_ref.shape
    rows = rows_ref.shape[0]
    group, core = lax.axis_index("dp"), lax.axis_index("vocab")
    cores = lax.axis_size("vocab")
    at = 0
    for c, order in enumerate(plan):
        early, late = pieces[2 * c : 2 * c + 2]
        width = early.shape[1]
        for j in range(rows // SUB):
            to = place(order, j) * SUB
            ref = early if j < rows // SUB // 2 else late
            at_row = j * SUB % (rows // 2)
            rows_ref[to : to + SUB, at : at + width] = ref[at_row : at_row + SUB, :]
        at += width
    states = rows_ref[:, :features]

    def multiply(n, top):
        columns = pl.ds(pl.multiple_of(n * TILE, TILE), TILE)
        part = jnp.dot(
            states, weight_ref[:, columns], preferred_element_type=jnp.float32
        )
        logits_ref[:, columns] = part
        for k in range(TILE // LANES):
            top = jnp.maximum(top, part[:, k * LANES : (k + 1) * LANES])
        return top

    top = jnp.full((rows, LANES), -jnp.inf, jnp.float32)
    top = lax.fori_loop(0, vocab_cols // TILE, multiply, top, unroll=True)
    top = jnp.max(top, axis=1, keepdims=True)
    digits = rows_ref[:, features:].astype(jnp.float32)
    lane = lax.broadcasted_iota(jnp.int32, (rows, LANES), 1)
    scale = jnp.where(lane == 0, 1.0, jnp.where(lane == 1, 256.0, 65536.0))
    scale = jnp.where(lane < DIGITS, scale, 0.0)
    label = jnp.sum(digits * scale, axis=1, keepdims=True).astype(jnp.int32)
    start = (group * cores + core) * vocab_cols
    offset = lane + start - label

    total = jnp.zeros((rows, LANES), jnp.float32)
    picked = jnp.zeros((rows, LANES), jnp.float32)
    for n in range(vocab_cols // LANES):
        part = logits_ref[:, n * LANES : (n + 1) * LANES]
        total = total + jnp.exp(part - top)
        picked = picked + jnp.where(offset == -n * LANES, part, 0.0)
    norm = top + jnp.log(jnp.sum(total, axis=1, keepdims=True))
    picked = jnp.sum(picked, axis=1, keepdims=True)
    stats = jnp.where(lane == 0, norm, jnp.where(lane == 1, picked, 0.0))
    for j in range(rows // SUB):
        to = pl.multiple_of((group ^ j) * SUB, SUB)
        stats_ref[pl.ds(to, SUB), :] = stats[j * SUB : (j + 1) * SUB, :]
    stats = stats_ref[...].T[:2, :]
    if not flip:
        out_ref[...] = stats
        return
    before = before_ref[...]
    low = jnp.where(core == 0, before, stats)
    high = jnp.where(core == 0, stats, before)
    out_ref[:, 0:1, :] = jnp.broadcast_to(low[0:1][None], (out_ref.shape[0], 1, rows))
    out_ref[:, 1:2, :] = jnp.broadcast_to(high[0:1][None], (out_ref.shape[0], 1, rows))
    out_ref[:, 2:3, :] = jnp.broadcast_to(low[1:2][None], (out_ref.shape[0], 1, rows))
    out_ref[:, 3:4, :] = jnp.broadcast_to(high[1:2][None], (out_ref.shape[0], 1, rows))


def finish_kernel(share, stats_ref, token_ref, mean_ref):
    group = lax.axis_index("dp")
    stats = stats_ref[...]
    length = stats.shape[-1]
    top = jnp.max(stats, axis=0)
    total = jnp.sum(jnp.exp(stats - top[None]), axis=0)
    log_norm = top + jnp.log(total)
    picked = jnp.sum(stats, axis=0)
    loss = log_norm[0:2] - picked[2:4]
    mean_ref[...] = jnp.sum(loss, keepdims=True) / (2 * length)
    lane = lax.broadcasted_iota(jnp.int32, (1, length), 1)
    low = pltpu.roll(loss[0:1], (length - group * share) % length, 1)
    high = pltpu.roll(loss[1:2], (length + share - group * share) % length, 1)
    token_ref[...] = jnp.where(lane < share, low, high)[:, : 2 * share]


def shards(hidden_states, targets, out_weight):
    features, vocab_cols = out_weight.shape
    local_tokens = hidden_states.shape[0]
    groups, cores = lax.axis_size("dp"), lax.axis_size("vocab")
    share = local_tokens // cores
    half = groups * share
    dtype = hidden_states.dtype
    plan = orders(groups)
    cut = features // len(plan) // LANES * LANES
    widths = [cut] * (len(plan) - 1)
    widths.append(features - sum(widths) + LANES)

    pieces = pl.pallas_call(
        functools.partial(pack_kernel, share),
        out_shape=[jax.ShapeDtypeStruct((share, w), dtype) for w in widths],
        in_specs=[HBM, HBM],
        out_specs=[VMEM] * len(widths),
        scratch_shapes=[
            pltpu.SMEM((local_tokens,), jnp.int32),
            pltpu.VMEM((share, features), dtype),
            pltpu.SemaphoreType.DMA((2,)),
        ],
        compiler_params=LIMIT,
        name="pack",
    )(far(targets), far(hidden_states))

    steps = len(plan[0])
    weight = None
    unit = SUB * CHUNKS
    first = int(features * SHARE) // unit * unit
    spans = {STEPS[0]: (0, first), steps - STEPS[1]: (first, features - first)}
    spans = {s: v for s, v in spans.items() if v[1]}
    joined = steps - 2
    whole = jnp.concatenate(pieces, axis=1)
    for step in range(0, joined, 2):
        bits = plan[0][step : step + 2]
        parts = {}
        for n in ORDER:
            if n < 1 << len(bits):
                k = place(bits, n)
                flips = [(i, i ^ k) for i in range(groups)]
                parts[n] = lax.ppermute(whole, "dp", flips)
        if step in spans:
            weight, whole = load(spans[step], out_weight, whole, weight)
        parts[0] = whole
        whole = jnp.concatenate([parts[n] for n in range(len(parts))], axis=0)
    mine = [[whole[:, :cut]], [whole[:, cut:]]]
    for step in range(joined, steps):
        for c, order in enumerate(plan):
            flips = [(i, i ^ order[step]) for i in range(groups)]
            whole = jnp.concatenate(mine[c], axis=0)
            mine[c] = [whole, lax.ppermute(whole, "dp", flips)]
        if step in spans:
            weight, mine[-1][0] = load(spans[step], out_weight, whole, weight)
    mine = [part for pair in mine for part in pair]
    swap = [(i, (i + 1) % cores) for i in range(cores)]
    other = [lax.ppermute(part, "vocab", swap) for part in mine]

    weight = near(weight)
    cost = pl.CostEstimate(
        flops=2 * half * features * vocab_cols,
        bytes_accessed=2 * half * features,
        transcendentals=half * vocab_cols,
    )

    def score(pieces, before):
        flip = before is not None
        shape = (groups * cores, 4, half) if flip else (2, half)
        extra = [before] if flip else []
        return pl.pallas_call(
            functools.partial(score_kernel, plan, flip),
            out_shape=jax.ShapeDtypeStruct(shape, jnp.float32),
            in_specs=[VMEM] * (len(pieces) + 1 + len(extra)),
            out_specs=VMEM,
            scratch_shapes=[
                pltpu.VMEM((half, features + LANES), dtype),
                pltpu.VMEM((half, vocab_cols), jnp.float32),
                pltpu.VMEM((half, LANES), jnp.float32),
            ],
            cost_estimate=cost,
            compiler_params=LIMIT,
            name="score_other" if flip else "score_mine",
        )(*[near(p) for p in pieces], weight, *extra)

    stats = score(other, score(mine, None))
    stats = lax.all_to_all(stats, ("dp", "vocab"), 0, 0)
    token_loss, loss_mean = pl.pallas_call(
        functools.partial(finish_kernel, share),
        out_shape=[
            jax.ShapeDtypeStruct((1, local_tokens), jnp.float32),
            jax.ShapeDtypeStruct((1, 1), jnp.float32),
        ],
        in_specs=[VMEM],
        out_specs=[VMEM, VMEM],
        compiler_params=LIMIT,
        name="finish",
    )(stats)
    return token_loss.reshape(local_tokens), loss_mean.reshape(())


def solution(mesh):
    placed = (P("dp", None), P("dp"), P(None, ("dp", "vocab")))
    return jax.shard_map(
        shards, mesh=mesh, in_specs=placed, out_specs=(P("dp"), P()), check_vma=False
    )
```

```python
import functools

import jax
import jax.numpy as jnp
from jax import lax
from jax.experimental import pallas as pl
from jax.experimental.pallas import tpu as pltpu
from jax.sharding import PartitionSpec as P

LANES = 128
SUB = 8
BASE = 256
DIGITS = 3
PARTS = 4
ORDER = (1, 2, 3)
SHARE = 0.5
STEPS = (0, 1)
TILE = 256
VMEM = pl.BlockSpec(memory_space=pltpu.VMEM)
LIMIT = pltpu.CompilerParams(vmem_limit_bytes=20 * 2**20)
HBM = pl.BlockSpec(memory_space=pltpu.HBM)
CHUNKS = 8


def near(array):
    return pltpu.with_memory_space_constraint(array, pltpu.VMEM)


def far(array):
    return pltpu.with_memory_space_constraint(array, pltpu.HBM)


def orders(groups):
    bits = [1 << b for b in reversed(range(groups.bit_length() - 1))]
    return bits


def place(order, j):
    where = 0
    for b, k in enumerate(order):
        where ^= k * ((j >> b) & 1)
    return where


def pack_kernel(share, targets_hbm, states_hbm, *refs):
    piece_refs, (targets_ref, states_ref, sems) = refs[:-3], refs[-3:]
    core = lax.axis_index("vocab")
    first = pl.multiple_of(core * share, share)
    copies = (
        pltpu.make_async_copy(targets_hbm, targets_ref, sems.at[0]),
        pltpu.make_async_copy(
            states_hbm.at[pl.ds(first, share), :], states_ref, sems.at[1]
        ),
    )
    for copy in copies:
        copy.start()
    for copy in copies:
        copy.wait()
    block = states_ref[...]
    row = lax.broadcasted_iota(jnp.int32, (share, LANES), 0)
    lane = lax.broadcasted_iota(jnp.int32, (share, LANES), 1)
    label = jnp.zeros((share, LANES), jnp.int32)
    for t in range(share):
        label = jnp.where(row == t, targets_ref[first + t], label)
    digits = jnp.zeros((share, LANES), jnp.int32)
    for d in range(DIGITS):
        digits = jnp.where(lane == d, (label >> (8 * d)) & (BASE - 1), digits)
    digits = digits.astype(jnp.float32).astype(block.dtype)
    at = 0
    for c, ref in enumerate(piece_refs):
        last = c == len(piece_refs) - 1
        width = ref.shape[1] - (LANES if last else 0)
        ref[:, :width] = block[:, at : at + width]
        at += width
        if last:
            ref[:, width:] = digits


def load_kernel(part, source, piece_ref, *refs):
    target, again_ref, sems = refs[-3:]
    first, size = part
    rows = size // CHUNKS
    copies = []
    for n in range(CHUNKS):
        span = pl.ds(first + n * rows, rows)
        copies.append(
            pltpu.make_async_copy(source.at[span], target.at[span], sems.at[n])
        )
        copies[-1].start()
    again_ref[...] = piece_ref[...]
    for copy in copies:
        copy.wait()


def load(part, source, piece, target):
    first = target is None
    return pl.pallas_call(
        functools.partial(load_kernel, part),
        out_shape=[
            jax.ShapeDtypeStruct(source.shape, source.dtype),
            jax.ShapeDtypeStruct(piece.shape, piece.dtype),
        ],
        in_specs=[HBM, VMEM] + ([] if first else [VMEM]),
        out_specs=[VMEM, VMEM],
        scratch_shapes=[pltpu.SemaphoreType.DMA((CHUNKS,))],
        input_output_aliases={} if first else {2: 0},
        compiler_params=LIMIT,
        cost_estimate=pl.CostEstimate(
            flops=2 * part[1] * source.shape[1] * 2 * LANES,
            bytes_accessed=0,
            transcendentals=0,
        ),
        name=f"load_{part[0]}",
    )(far(source), piece, *([] if first else [near(target)]))


def score_kernel(plan, flip, *refs):
    pieces, rest = refs[:PARTS], list(refs[PARTS:])
    weight_ref = rest.pop(0)
    before_ref = rest.pop(0) if flip else None
    out_ref, rows_ref, logits_ref, stats_ref = rest
    features, vocab_cols = weight_ref.shape
    rows = rows_ref.shape[0]
    group, core = lax.axis_index("dp"), lax.axis_index("vocab")
    cores = lax.axis_size("vocab")
    size = rows // len(pieces)
    for n, ref in enumerate(pieces):
        rows_ref[n * size : (n + 1) * size, :] = ref[...]
    states = rows_ref[:, :features]

    def multiply(n, top):
        columns = pl.ds(pl.multiple_of(n * TILE, TILE), TILE)
        part = jnp.dot(
            states, weight_ref[:, columns], preferred_element_type=jnp.float32
        )
        logits_ref[:, columns] = part
        for k in range(TILE // LANES):
            top = jnp.maximum(top, part[:, k * LANES : (k + 1) * LANES])
        return top

    top = jnp.full((rows, LANES), -jnp.inf, jnp.float32)
    top = lax.fori_loop(0, vocab_cols // TILE, multiply, top, unroll=True)
    top = jnp.max(top, axis=1, keepdims=True)
    digits = rows_ref[:, features:].astype(jnp.float32)
    lane = lax.broadcasted_iota(jnp.int32, (rows, LANES), 1)
    scale = jnp.where(lane == 0, 1.0, jnp.where(lane == 1, 256.0, 65536.0))
    scale = jnp.where(lane < DIGITS, scale, 0.0)
    label = jnp.sum(digits * scale, axis=1, keepdims=True).astype(jnp.int32)
    start = (group * cores + core) * vocab_cols
    offset = lane + start - label

    total = jnp.zeros((rows, LANES), jnp.float32)
    picked = jnp.zeros((rows, LANES), jnp.float32)
    for n in range(vocab_cols // LANES):
        part = logits_ref[:, n * LANES : (n + 1) * LANES]
        total = total + jnp.exp(part - top)
        picked = picked + jnp.where(offset == -n * LANES, part, 0.0)
    norm = top + jnp.log(jnp.sum(total, axis=1, keepdims=True))
    picked = jnp.sum(picked, axis=1, keepdims=True)
    stats = jnp.where(lane == 0, norm, jnp.where(lane == 1, picked, 0.0))
    for j in range(rows // SUB):
        to = pl.multiple_of((group ^ place(plan, j)) * SUB, SUB)
        stats_ref[pl.ds(to, SUB), :] = stats[j * SUB : (j + 1) * SUB, :]
    stats = stats_ref[...].T[:2, :]
    if not flip:
        out_ref[...] = stats
        return
    before = before_ref[...]
    low = jnp.where(core == 0, before, stats)
    high = jnp.where(core == 0, stats, before)
    out_ref[:, 0:1, :] = jnp.broadcast_to(low[0:1][None], (out_ref.shape[0], 1, rows))
    out_ref[:, 1:2, :] = jnp.broadcast_to(high[0:1][None], (out_ref.shape[0], 1, rows))
    out_ref[:, 2:3, :] = jnp.broadcast_to(low[1:2][None], (out_ref.shape[0], 1, rows))
    out_ref[:, 3:4, :] = jnp.broadcast_to(high[1:2][None], (out_ref.shape[0], 1, rows))


def finish_kernel(share, stats_ref, token_ref, mean_ref):
    group = lax.axis_index("dp")
    stats = stats_ref[...]
    length = stats.shape[-1]
    top = jnp.max(stats, axis=0)
    total = jnp.sum(jnp.exp(stats - top[None]), axis=0)
    log_norm = top + jnp.log(total)
    picked = jnp.sum(stats, axis=0)
    loss = log_norm[0:2] - picked[2:4]
    mean_ref[...] = jnp.sum(loss, keepdims=True) / (2 * length)
    lane = lax.broadcasted_iota(jnp.int32, (1, length), 1)
    low = pltpu.roll(loss[0:1], (length - group * share) % length, 1)
    high = pltpu.roll(loss[1:2], (length + share - group * share) % length, 1)
    token_ref[...] = jnp.where(lane < share, low, high)[:, : 2 * share]


def shards(hidden_states, targets, out_weight):
    features, vocab_cols = out_weight.shape
    local_tokens = hidden_states.shape[0]
    groups, cores = lax.axis_size("dp"), lax.axis_size("vocab")
    share = local_tokens // cores
    half = groups * share
    dtype = hidden_states.dtype
    plan = orders(groups)
    width = features + LANES

    pieces = pl.pallas_call(
        functools.partial(pack_kernel, share),
        out_shape=[jax.ShapeDtypeStruct((share, width), dtype)],
        in_specs=[HBM, HBM],
        out_specs=[VMEM],
        scratch_shapes=[
            pltpu.SMEM((local_tokens,), jnp.int32),
            pltpu.VMEM((share, features), dtype),
            pltpu.SemaphoreType.DMA((2,)),
        ],
        compiler_params=LIMIT,
        name="pack",
    )(far(targets), far(hidden_states))

    steps = len(plan)
    weight = None
    unit = SUB * CHUNKS
    first = int(features * SHARE) // unit * unit
    spans = {0: (0, first), steps - 2: (first, features - first)}
    (whole,) = pieces
    for step in range(0, steps, 2):
        bits = plan[step : step + 2]
        mine = [whole]
        for n in range(1, 1 << len(bits)):
            k = place(bits, n)
            flips = [(i, i ^ k) for i in range(groups)]
            mine.append(lax.ppermute(whole, "dp", flips))
        if step in spans:
            weight, mine[0] = load(spans[step], out_weight, whole, weight)
        if step + 2 < steps:
            whole = jnp.concatenate(mine, axis=0)
    swap = [(i, (i + 1) % cores) for i in range(cores)]
    other = [lax.ppermute(part, "vocab", swap) for part in mine]

    weight = near(weight)
    cost = pl.CostEstimate(
        flops=2 * half * features * vocab_cols,
        bytes_accessed=2 * half * features,
        transcendentals=half * vocab_cols,
    )

    def score(pieces, before):
        flip = before is not None
        shape = (groups * cores, 4, half) if flip else (2, half)
        extra = [before] if flip else []
        return pl.pallas_call(
            functools.partial(score_kernel, plan, flip),
            out_shape=jax.ShapeDtypeStruct(shape, jnp.float32),
            in_specs=[VMEM] * (len(pieces) + 1 + len(extra)),
            out_specs=VMEM,
            scratch_shapes=[
                pltpu.VMEM((half, features + LANES), dtype),
                pltpu.VMEM((half, vocab_cols), jnp.float32),
                pltpu.VMEM((half, LANES), jnp.float32),
            ],
            cost_estimate=cost,
            compiler_params=LIMIT,
            name="score_other" if flip else "score_mine",
        )(*[near(p) for p in pieces], weight, *extra)

    stats = score(other, score(mine, None))
    stats = lax.all_to_all(stats, ("dp", "vocab"), 0, 0)
    token_loss, loss_mean = pl.pallas_call(
        functools.partial(finish_kernel, share),
        out_shape=[
            jax.ShapeDtypeStruct((1, local_tokens), jnp.float32),
            jax.ShapeDtypeStruct((1, 1), jnp.float32),
        ],
        in_specs=[VMEM],
        out_specs=[VMEM, VMEM],
        compiler_params=LIMIT,
        name="finish",
    )(stats)
    return token_loss.reshape(local_tokens), loss_mean.reshape(())


def solution(mesh):
    placed = (P("dp", None), P("dp"), P(None, ("dp", "vocab")))
    return jax.shard_map(
        shards, mesh=mesh, in_specs=placed, out_specs=(P("dp"), P()), check_vma=False
    )
```

```python
import functools

import jax
import jax.numpy as jnp
from jax import lax
from jax.experimental import pallas as pl
from jax.experimental.pallas import tpu as pltpu
from jax.sharding import PartitionSpec as P

LANES = 128
SUB = 8
BASE = 256
DIGITS = 3
PARTS = 4
ORDER = (1, 2, 3)
SHARE = 0.3
STEPS = (0, 1)
TILE = 256
VMEM = pl.BlockSpec(memory_space=pltpu.VMEM)
LIMIT = pltpu.CompilerParams(vmem_limit_bytes=20 * 2**20)
HBM = pl.BlockSpec(memory_space=pltpu.HBM)
CHUNKS = 8


def near(array):
    return pltpu.with_memory_space_constraint(array, pltpu.VMEM)


def far(array):
    return pltpu.with_memory_space_constraint(array, pltpu.HBM)


def orders(groups):
    bits = [1 << b for b in reversed(range(groups.bit_length() - 1))]
    return bits


def place(order, j):
    where = 0
    for b, k in enumerate(order):
        where ^= k * ((j >> b) & 1)
    return where


def pack_kernel(share, targets_hbm, states_hbm, *refs):
    piece_refs, (targets_ref, states_ref, sems) = refs[:-3], refs[-3:]
    core = lax.axis_index("vocab")
    first = pl.multiple_of(core * share, share)
    copies = (
        pltpu.make_async_copy(targets_hbm, targets_ref, sems.at[0]),
        pltpu.make_async_copy(
            states_hbm.at[pl.ds(first, share), :], states_ref, sems.at[1]
        ),
    )
    for copy in copies:
        copy.start()
    for copy in copies:
        copy.wait()
    block = states_ref[...]
    row = lax.broadcasted_iota(jnp.int32, (share, LANES), 0)
    lane = lax.broadcasted_iota(jnp.int32, (share, LANES), 1)
    label = jnp.zeros((share, LANES), jnp.int32)
    for t in range(share):
        label = jnp.where(row == t, targets_ref[first + t], label)
    digits = jnp.zeros((share, LANES), jnp.int32)
    for d in range(DIGITS):
        digits = jnp.where(lane == d, (label >> (8 * d)) & (BASE - 1), digits)
    digits = digits.astype(jnp.float32).astype(block.dtype)
    at = 0
    for c, ref in enumerate(piece_refs):
        last = c == len(piece_refs) - 1
        width = ref.shape[1] - (LANES if last else 0)
        ref[:, :width] = block[:, at : at + width]
        at += width
        if last:
            ref[:, width:] = digits


def load_kernel(part, source, piece_ref, *refs):
    target, again_ref, sems = refs[-3:]
    first, size = part
    rows = size // CHUNKS
    copies = []
    for n in range(CHUNKS):
        span = pl.ds(first + n * rows, rows)
        copies.append(
            pltpu.make_async_copy(source.at[span], target.at[span], sems.at[n])
        )
        copies[-1].start()
    again_ref[...] = piece_ref[...]
    for copy in copies:
        copy.wait()


def load(part, source, piece, target):
    first = target is None
    return pl.pallas_call(
        functools.partial(load_kernel, part),
        out_shape=[
            jax.ShapeDtypeStruct(source.shape, source.dtype),
            jax.ShapeDtypeStruct(piece.shape, piece.dtype),
        ],
        in_specs=[HBM, VMEM] + ([] if first else [VMEM]),
        out_specs=[VMEM, VMEM],
        scratch_shapes=[pltpu.SemaphoreType.DMA((CHUNKS,))],
        input_output_aliases={} if first else {2: 0},
        compiler_params=LIMIT,
        cost_estimate=pl.CostEstimate(
            flops=2 * part[1] * source.shape[1] * 2 * LANES,
            bytes_accessed=0,
            transcendentals=0,
        ),
        name=f"load_{part[0]}",
    )(far(source), piece, *([] if first else [near(target)]))


def score_kernel(plan, flip, *refs):
    pieces, rest = refs[:PARTS], list(refs[PARTS:])
    weight_ref = rest.pop(0)
    before_ref = rest.pop(0) if flip else None
    out_ref, rows_ref, logits_ref, stats_ref = rest
    features, vocab_cols = weight_ref.shape
    rows = rows_ref.shape[0]
    group, core = lax.axis_index("dp"), lax.axis_index("vocab")
    cores = lax.axis_size("vocab")
    size = rows // len(pieces)
    for n, ref in enumerate(pieces):
        rows_ref[n * size : (n + 1) * size, :] = ref[...]
    states = rows_ref[:, :features]

    def multiply(n, top):
        columns = pl.ds(pl.multiple_of(n * TILE, TILE), TILE)
        part = jnp.dot(
            states, weight_ref[:, columns], preferred_element_type=jnp.float32
        )
        logits_ref[:, columns] = part
        for k in range(TILE // LANES):
            top = jnp.maximum(top, part[:, k * LANES : (k + 1) * LANES])
        return top

    top = jnp.full((rows, LANES), -jnp.inf, jnp.float32)
    top = lax.fori_loop(0, vocab_cols // TILE, multiply, top, unroll=True)
    top = jnp.max(top, axis=1, keepdims=True)
    digits = rows_ref[:, features:].astype(jnp.float32)
    lane = lax.broadcasted_iota(jnp.int32, (rows, LANES), 1)
    scale = jnp.where(lane == 0, 1.0, jnp.where(lane == 1, 256.0, 65536.0))
    scale = jnp.where(lane < DIGITS, scale, 0.0)
    label = jnp.sum(digits * scale, axis=1, keepdims=True).astype(jnp.int32)
    start = (group * cores + core) * vocab_cols
    offset = lane + start - label

    total = jnp.zeros((rows, LANES), jnp.float32)
    picked = jnp.zeros((rows, LANES), jnp.float32)
    for n in range(vocab_cols // LANES):
        part = logits_ref[:, n * LANES : (n + 1) * LANES]
        total = total + jnp.exp(part - top)
        picked = picked + jnp.where(offset == -n * LANES, part, 0.0)
    norm = top + jnp.log(jnp.sum(total, axis=1, keepdims=True))
    picked = jnp.sum(picked, axis=1, keepdims=True)
    stats = jnp.where(lane == 0, norm, jnp.where(lane == 1, picked, 0.0))
    for j in range(rows // SUB):
        to = pl.multiple_of((group ^ place(plan, j)) * SUB, SUB)
        stats_ref[pl.ds(to, SUB), :] = stats[j * SUB : (j + 1) * SUB, :]
    stats = stats_ref[...].T[:2, :]
    if not flip:
        out_ref[...] = stats
        return
    before = before_ref[...]
    low = jnp.where(core == 0, before, stats)
    high = jnp.where(core == 0, stats, before)
    out_ref[:, 0:1, :] = jnp.broadcast_to(low[0:1][None], (out_ref.shape[0], 1, rows))
    out_ref[:, 1:2, :] = jnp.broadcast_to(high[0:1][None], (out_ref.shape[0], 1, rows))
    out_ref[:, 2:3, :] = jnp.broadcast_to(low[1:2][None], (out_ref.shape[0], 1, rows))
    out_ref[:, 3:4, :] = jnp.broadcast_to(high[1:2][None], (out_ref.shape[0], 1, rows))


def finish_kernel(share, stats_ref, token_ref, mean_ref):
    group = lax.axis_index("dp")
    stats = stats_ref[...]
    length = stats.shape[-1]
    top = jnp.max(stats, axis=0)
    total = jnp.sum(jnp.exp(stats - top[None]), axis=0)
    log_norm = top + jnp.log(total)
    picked = jnp.sum(stats, axis=0)
    loss = log_norm[0:2] - picked[2:4]
    mean_ref[...] = jnp.sum(loss, keepdims=True) / (2 * length)
    lane = lax.broadcasted_iota(jnp.int32, (1, length), 1)
    low = pltpu.roll(loss[0:1], (length - group * share) % length, 1)
    high = pltpu.roll(loss[1:2], (length + share - group * share) % length, 1)
    token_ref[...] = jnp.where(lane < share, low, high)[:, : 2 * share]


def shards(hidden_states, targets, out_weight):
    features, vocab_cols = out_weight.shape
    local_tokens = hidden_states.shape[0]
    groups, cores = lax.axis_size("dp"), lax.axis_size("vocab")
    share = local_tokens // cores
    half = groups * share
    dtype = hidden_states.dtype
    plan = orders(groups)
    width = features + LANES

    pieces = pl.pallas_call(
        functools.partial(pack_kernel, share),
        out_shape=[jax.ShapeDtypeStruct((share, width), dtype)],
        in_specs=[HBM, HBM],
        out_specs=[VMEM],
        scratch_shapes=[
            pltpu.SMEM((local_tokens,), jnp.int32),
            pltpu.VMEM((share, features), dtype),
            pltpu.SemaphoreType.DMA((2,)),
        ],
        compiler_params=LIMIT,
        name="pack",
    )(far(targets), far(hidden_states))

    steps = len(plan)
    weight = None
    unit = SUB * CHUNKS
    first = int(features * SHARE) // unit * unit
    spans = {0: (0, first), steps - 2: (first, features - first)}
    (whole,) = pieces
    for step in range(0, steps, 2):
        bits = plan[step : step + 2]
        mine = [whole]
        for n in range(1, 1 << len(bits)):
            k = place(bits, n)
            flips = [(i, i ^ k) for i in range(groups)]
            mine.append(lax.ppermute(whole, "dp", flips))
        if step in spans:
            weight, mine[0] = load(spans[step], out_weight, whole, weight)
        if step + 2 < steps:
            whole = jnp.concatenate(mine, axis=0)
    swap = [(i, (i + 1) % cores) for i in range(cores)]
    other = [lax.ppermute(part, "vocab", swap) for part in mine]

    weight = near(weight)
    cost = pl.CostEstimate(
        flops=2 * half * features * vocab_cols,
        bytes_accessed=2 * half * features,
        transcendentals=half * vocab_cols,
    )

    def score(pieces, before):
        flip = before is not None
        shape = (groups * cores, 4, half) if flip else (2, half)
        extra = [before] if flip else []
        return pl.pallas_call(
            functools.partial(score_kernel, plan, flip),
            out_shape=jax.ShapeDtypeStruct(shape, jnp.float32),
            in_specs=[VMEM] * (len(pieces) + 1 + len(extra)),
            out_specs=VMEM,
            scratch_shapes=[
                pltpu.VMEM((half, features + LANES), dtype),
                pltpu.VMEM((half, vocab_cols), jnp.float32),
                pltpu.VMEM((half, LANES), jnp.float32),
            ],
            cost_estimate=cost,
            compiler_params=LIMIT,
            name="score_other" if flip else "score_mine",
        )(*[near(p) for p in pieces], weight, *extra)

    stats = score(other, score(mine, None))
    stats = lax.all_to_all(stats, ("dp", "vocab"), 0, 0)
    token_loss, loss_mean = pl.pallas_call(
        functools.partial(finish_kernel, share),
        out_shape=[
            jax.ShapeDtypeStruct((1, local_tokens), jnp.float32),
            jax.ShapeDtypeStruct((1, 1), jnp.float32),
        ],
        in_specs=[VMEM],
        out_specs=[VMEM, VMEM],
        compiler_params=LIMIT,
        name="finish",
    )(stats)
    return token_loss.reshape(local_tokens), loss_mean.reshape(())


def solution(mesh):
    placed = (P("dp", None), P("dp"), P(None, ("dp", "vocab")))
    return jax.shard_map(
        shards, mesh=mesh, in_specs=placed, out_specs=(P("dp"), P()), check_vma=False
    )
```
